1024 devices in a mesh: group: 16 (over y, core), member: 64 (over z, x).
Axes of the slice: x: 4, y: 8, z: 16, core: 2. Of those that a mesh axis runs over, the one named last changes fastest.
Arguments:
- off_tiles: bfloat16 [2048, 8, 128, 128], P(('group', 'member')), may hold values from -0.1875 to 0.1875
- off_cols: int32 [2048, 8], P(('group', 'member')), may hold values from 0 to 73
- member_send: int32 [1024, 64, 1], P(('group', 'member')), may hold values from 0 to 1
- group_send: int32 [1024, 4], P(('group', 'member')), may hold values from 0 to 1
- diag_tiles: bfloat16 [2048, 128, 128], P(('group', 'member')), may hold values from -1 to 9
- smoother: bfloat16 [2048, 128, 128], P(('group', 'member')), may hold values from -1 to 1
- agg_map: int32 [2048], P(('group', 'member')), may hold values from 0 to 1
- prolong: bfloat16 [2048, 128, 128], P(('group', 'member')), may hold values from -0.5 to 0.5
- coarse_inv: bfloat16 [4096, 4096], P(None, 'group'), may hold values from -0.005859375 to 0.005859375
- krylov_basis: bfloat16 [2048, 32, 128], P(('group', 'member')), may hold values from -24 to 24, as said below
Outputs:
- preconditioned: bfloat16 [2048, 8, 128], P(('group', 'member'))
- coefficients: float32 [32, 8], replicated
- gram_matrix: float32 [8, 8], replicated
- new_block: float32 [2048, 8, 128], P(('group', 'member'))
The draws below stay inside these ranges and needn't reach their ends.
Inputs may be any that keep to these rules, and one draw needn't show every extreme that they name: `off_cols`: entries below 2 name the device's own row tiles; entry 2 + p + s names slot s of what member p of the same group sends; the last 8 entries name what the groups below and above send. `member_send`: entry [d, p, s] is the local row tile that device d sends to member p of its group in slot s. `group_send`: entry [d, s] is the local row tile that device d sends, in slot s, to the same member of the groups below and above. `krylov_basis`: the 32 basis vectors are orthonormal, up to bfloat16 rounding, under the inner product (1 / 262144) times the sum over all rows.
All inputs are finite; a program needn't handle non-finite values.
Results may differ from the reference program's by a relative error of at most 0.02.
Values may be sent and summed in bfloat16 or wider, within the bound.
A program may use at most 32 MiB of HBM per device.

```python
import math
import jax
import jax.numpy as jnp
from jax import lax

TILE = 128
NVEC = 8
K = 8
GH = 1
GG = 4
CTG = 2
TD = 2
NT = 2048
ROWS = 262144
NB = 32
NCT = 32
NC = 4096
N_GROUP = 16
N_MEMBER = 64


def pivot_values(key):
    logs = jax.random.uniform(jax.random.fold_in(key, 11), (NT, TILE), jnp.float32, math.log(2.0), math.log(6.0))
    return jnp.exp(logs)


def draw_diag_tiles(key, part):
    pivots = pivot_values(key)
    noise = jnp.clip(jax.random.normal(jax.random.fold_in(key, 12), (NT, TILE, TILE), jnp.float32), -6.0, 6.0)
    noise = noise * (0.8 / math.sqrt(TILE))
    identity = jnp.eye(TILE, dtype=jnp.float32)
    return (noise + identity[None, :, :] * pivots[:, :, None]).astype(jnp.bfloat16)


def draw_smoother(key, part):
    pivots = pivot_values(key)
    noise = jnp.clip(jax.random.normal(jax.random.fold_in(key, 13), (NT, TILE, TILE), jnp.float32), -6.0, 6.0)
    noise = noise * (0.1 / math.sqrt(TILE))
    identity = jnp.eye(TILE, dtype=jnp.float32)
    return (0.7 * (noise + identity[None, :, :] / pivots[:, :, None])).astype(jnp.bfloat16)


def draw_krylov_basis(key, part):
    position = jnp.arange(NT, dtype=jnp.float32) / (NT - 1)
    rough = jnp.exp(jax.random.uniform(jax.random.fold_in(key, 21), (NT, NB, 1), jnp.float32, 0.0, math.log(2.0)))
    ramp = 1.0 + 2.0 * position
    base = jnp.clip(jax.random.normal(jax.random.fold_in(key, 22), (NT, NB, TILE), jnp.float32), -4.0, 4.0)
    values = base * ramp[:, None, None] * rough
    matrix = jnp.transpose(values, (0, 2, 1)).reshape(NT * TILE, NB)
    ortho, upper = jnp.linalg.qr(matrix)
    ortho = ortho * math.sqrt(NT * TILE)
    values = jnp.transpose(ortho.reshape(NT, TILE, NB), (0, 2, 1))
    return jnp.clip(values, -24.0, 24.0).astype(jnp.bfloat16)


def place_ends(values, key, smallest, top_value):
    longest = values.shape.index(max(values.shape))
    spots = []
    for shift in (0, 1):
        where = [jax.random.randint(jax.random.fold_in(key, axis), (), 0, length) for axis, length in enumerate(values.shape)]
        where[longest] = (where[longest] + shift) % values.shape[longest]
        spots.append(tuple(where))
    return values.at[spots[0]].set(smallest).at[spots[1]].set(top_value)


def block_scale(own_key, shape, cuts, low, largest):
    gain = 1.0
    for axis_at, parts in cuts:
        heights = jax.random.uniform(jax.random.fold_in(jax.random.fold_in(own_key, 6), axis_at), (parts,), jnp.float32, low / len(cuts), largest / len(cuts))
        gain = gain * jnp.repeat(jnp.exp(heights), shape[axis_at] // parts).reshape((-1,) + (1,) * (len(shape) - 1 - axis_at))
    return gain


def centred(rng, dims, width, reach, split=(), kind=jnp.bfloat16):
    array = width * jax.random.normal(rng, dims, jnp.float32)
    if split:
        array = array * block_scale(rng, dims, split, -0.22, 0.18)
    return jnp.clip(array, -reach, reach).astype(kind)


def setup_inputs(seed: int = 0) -> dict:
    seeds = jax.random.split(jax.random.key(seed), 11)
    return {
        "off_tiles": centred(seeds[0], (NT, K, TILE, TILE), (K * TILE) ** -0.5, 0.1875, ((0, 1024),)),
        "off_cols": place_ends(jax.random.randint(seeds[1], (NT, K), 0, TD + N_MEMBER * GH + 2 * GG), jax.random.fold_in(seeds[1], 1), 0, (TD + N_MEMBER * GH + 2 * GG) - 1).astype(jnp.int32),
        "member_send": place_ends(jax.random.randint(seeds[2], (N_GROUP * N_MEMBER, N_MEMBER, GH), 0, TD), jax.random.fold_in(seeds[2], 1), 0, TD - 1).astype(jnp.int32),
        "group_send": place_ends(jax.random.randint(seeds[3], (N_GROUP * N_MEMBER, GG), 0, TD), jax.random.fold_in(seeds[3], 1), 0, TD - 1).astype(jnp.int32),
        "diag_tiles": draw_diag_tiles(jax.random.fold_in(seeds[10], 71), 0),
        "smoother": draw_smoother(jax.random.fold_in(seeds[10], 71), 0),
        "agg_map": place_ends(jax.random.randint(seeds[6], (NT,), 0, CTG), jax.random.fold_in(seeds[6], 1), 0, CTG - 1).astype(jnp.int32),
        "prolong": centred(seeds[7], (NT, TILE, TILE), TILE ** -0.5, 0.5, ((0, 1024),)),
        "coarse_inv": centred(seeds[8], (NC, NC), (4 * NC * TD * N_MEMBER // CTG) ** -0.5, 0.005859375, ((1, 16),)),
        "krylov_basis": draw_krylov_basis(jax.random.fold_in(seeds[10], 71), 0),
    }


def ghost_sources(member_send, group_send):
    devices = N_GROUP * N_MEMBER
    device_ids = jnp.arange(devices, dtype=jnp.int32)
    group_ids = device_ids // N_MEMBER
    member_ids = device_ids % N_MEMBER
    own_tiles = device_ids[:, None] * TD + jnp.arange(TD, dtype=jnp.int32)[None, :]
    peer_ids = group_ids[:, None] * N_MEMBER + jnp.arange(N_MEMBER, dtype=jnp.int32)[None, :]
    slot_ids = member_send[peer_ids, member_ids[:, None], :]
    remote = (peer_ids[:, :, None] * TD + slot_ids).reshape(devices, N_MEMBER * GH)
    below = jnp.maximum(device_ids - N_MEMBER, 0)
    above = jnp.minimum(device_ids + N_MEMBER, devices - 1)
    lower_tiles = jnp.where(group_ids[:, None] > 0, below[:, None] * TD + group_send[below], NT)
    upper_tiles = jnp.where(group_ids[:, None] < N_GROUP - 1, above[:, None] * TD + group_send[above], NT)
    return jnp.concatenate([own_tiles, remote, lower_tiles, upper_tiles], axis=1).astype(jnp.int32)

def operate(values, off_tiles, global_cols, diag_tiles):
    padded = jnp.concatenate([values, jnp.zeros((1, NVEC, TILE), values.dtype)], axis=0)

    def per_device(device):
        offset = (device * TD).astype(jnp.int32)
        columns = lax.dynamic_slice_in_dim(global_cols, offset, TD, 0)
        tiles = lax.dynamic_slice_in_dim(off_tiles, offset, TD, 0).astype(jnp.float32)
        picked = padded[columns].astype(jnp.float32)
        own_part = lax.dynamic_slice_in_dim(values, offset, TD, 0).astype(jnp.float32)
        diagonal = lax.dynamic_slice_in_dim(diag_tiles, offset, TD, 0).astype(jnp.float32)
        far_part = jnp.einsum('tkcj,tkji->tci', picked, tiles, precision=lax.Precision.HIGHEST)
        near_part = jnp.einsum('tcj,tji->tci', own_part, diagonal, precision=lax.Precision.HIGHEST)
        return near_part + far_part
    result = lax.map(per_device, jnp.arange(N_GROUP * N_MEMBER, dtype=jnp.int32))
    return result.reshape(NT, NVEC, TILE)

def tilewise(left_side, tiles):
    return jnp.einsum('tcj,tji->tci', left_side.astype(jnp.float32), tiles.astype(jnp.float32), precision=lax.Precision.HIGHEST)

def reference(off_tiles, off_cols, member_send, group_send, diag_tiles, smoother, agg_map, prolong, coarse_inv, krylov_basis):
    sources = ghost_sources(member_send, group_send)
    owners = jnp.arange(NT, dtype=jnp.int32) // TD
    global_cols = sources[owners[:, None], off_cols].astype(jnp.int32)
    last_block = krylov_basis[:, NB - NVEC:, :]
    block_wide = last_block.astype(jnp.float32)
    first = tilewise(last_block, smoother).astype(jnp.bfloat16)
    residual_one = (block_wide - operate(first, off_tiles, global_cols, diag_tiles)).astype(jnp.bfloat16)
    pieces = jnp.einsum('tci,tji->tcj', residual_one.astype(jnp.float32), prolong.astype(jnp.float32), precision=lax.Precision.HIGHEST)
    coarse_ids = (jnp.arange(NT, dtype=jnp.int32) // (TD * N_MEMBER) * CTG + agg_map).astype(jnp.int32)
    coarse_rhs = jax.ops.segment_sum(pieces, coarse_ids, num_segments=NCT)
    coarse_round = coarse_rhs.astype(jnp.bfloat16)
    columns = coarse_inv.astype(jnp.float32).reshape(NCT, TILE, NC)
    correction = jnp.einsum('acj,ajo->co', coarse_round.astype(jnp.float32), columns, precision=lax.Precision.HIGHEST)
    correction = correction.astype(jnp.bfloat16).reshape(NVEC, NCT, TILE)
    chosen = jnp.transpose(correction[:, coarse_ids, :], (1, 0, 2))
    second = (first.astype(jnp.float32) + tilewise(chosen, prolong)).astype(jnp.bfloat16)
    residual_two = (block_wide - operate(second, off_tiles, global_cols, diag_tiles)).astype(jnp.bfloat16)
    preconditioned = (second.astype(jnp.float32) + tilewise(residual_two, smoother)).astype(jnp.bfloat16)
    applied = operate(preconditioned, off_tiles, global_cols, diag_tiles).astype(jnp.bfloat16)
    basis_wide = krylov_basis.astype(jnp.float32)
    coefficients = jnp.einsum('tpi,tci->pc', basis_wide, applied.astype(jnp.float32), precision=lax.Precision.HIGHEST) * (1.0 / ROWS)
    remainder = applied.astype(jnp.float32) - jnp.einsum('pc,tpi->tci', coefficients, basis_wide, precision=lax.Precision.HIGHEST)
    gram_matrix = jnp.einsum('tci,tdi->cd', remainder, remainder, precision=lax.Precision.HIGHEST) * (1.0 / ROWS)
    factor = jnp.linalg.cholesky(gram_matrix)
    inverse = lax.linalg.triangular_solve(factor, jnp.eye(NVEC, dtype=jnp.float32), left_side=True, lower=True)
    new_block = jnp.einsum('cd,tdi->tci', inverse, remainder, precision=lax.Precision.HIGHEST)
    return (preconditioned, coefficients, gram_matrix, new_block)
```

```python
import functools

import jax
import jax.numpy as jnp
from jax import lax
from jax.experimental import pallas as pl
from jax.experimental.pallas import tpu as pltpu
from jax.sharding import PartitionSpec as P

TILE = 128
NVEC = 8
NB = 32
CTG = 2
TD = 2
K = 8
GG = 4
NX = 4
F32 = jnp.float32
BF16 = jnp.bfloat16
HIGHEST = lax.Precision.HIGHEST
MESH = pl.DeviceIdType.MESH
NT_DIMS = (((1,), (1,)), ((), ()))


def dot(left, right):
    return jnp.dot(left, right, preferred_element_type=F32)


def dot_nt(left, right):
    return lax.dot_general(left, right, NT_DIMS, preferred_element_type=F32)


def exact(left, right):
    return jnp.dot(left, right, preferred_element_type=F32, precision=HIGHEST)


def exact_nt(left, right):
    return lax.dot_general(left, right, NT_DIMS, preferred_element_type=F32, precision=HIGHEST)


def cycle(
    groups, members, rows_all,
    off_cols, member_send, group_send, agg_map,
    off_hbm, diag_hbm, smooth_hbm, prolong_hbm, inv_hbm, basis_hbm,
    prec_ref, coef_ref, gram_ref, new_ref,
    off, diag, smooth, prolong, inv, basis,
    vals, out_tiles, out_rim, turn_0, turn_1, turn_2, ext_0, ext_1, ext_2,
    cx, cz, cg, corr,
    bz, bx, bg, fg, fx, fz,
    c_own, s_own, g_own, b_own, b2_own, b3_own, f_own, f2_own, f3_own,
    load_sem, turn_send, turn_recv, ex_send, ex_recv, st_send, st_recv,
):
    nz = members // NX
    ext = (ext_0, ext_1, ext_2)
    turn = (turn_0, turn_1, turn_2)
    g = lax.axis_index("group")
    m = lax.axis_index("member")
    z = lax.div(m, NX)
    x = lax.rem(m, NX)
    scale_rows = 1.0 / rows_all

    def at_member(pz, px):
        return {"group": g, "member": pz * NX + px}

    xs = [lax.rem(x + d, NX) for d in range(NX)]

    def z_of(k):
        return lax.rem(z + nz // 2 + lax.div(k + 1, 2) * (1 - 2 * lax.rem(k, 2)), nz)

    def each_z(act):
        def step(k, carry):
            act(z_of(k))
            return carry

        lax.fori_loop(0, nz - 1, step, 0)

    def each_group(act):
        def step(k, carry):
            act(lax.rem(g + 1 + k, groups))
            return carry

        lax.fori_loop(0, groups - 1, step, 0)

    barrier = pltpu.get_barrier_semaphore()
    each_z(
        lambda pz: pl.semaphore_signal(
            barrier, inc=1, device_id=at_member(pz, x), device_id_type=MESH
        )
    )
    for d in range(1, NX):
        pl.semaphore_signal(barrier, inc=1, device_id=at_member(z, xs[d]), device_id_type=MESH)
    each_group(
        lambda pg: pl.semaphore_signal(
            barrier, inc=1, device_id={"group": pg, "member": m}, device_id_type=MESH
        )
    )

    loads = [
        pltpu.make_async_copy(src, dst, load_sem.at[i])
        for i, (src, dst) in enumerate(
            (
                (basis_hbm, basis),
                (smooth_hbm, smooth),
                (off_hbm, off),
                (diag_hbm, diag),
                (prolong_hbm, prolong),
                (inv_hbm, inv),
            )
        )
    ]
    for load in loads:
        load.start()

    loads[0].wait()
    loads[1].wait()
    last = [basis[t, NB - NVEC :, :] for t in range(TD)]
    first = [dot(last[t], smooth[t]).astype(BF16) for t in range(TD)]

    def fill(r, tiles):
        for t in range(TD):
            vals[r, t] = tiles[t]
            ext[r][t] = tiles[t]

        def step(pz, carry):
            for px in range(NX):
                out_tiles[r, px, pz] = vals[r, member_send[pz * NX + px]]
            turn[r][x, pz] = vals[r, member_send[pz * NX + x]]
            return carry

        lax.fori_loop(0, nz, step, 0, unroll=True)
        for s in range(GG):
            out_rim[r, s] = vals[r, group_send[s]]

    def send_tiles(r):
        for d in (2, 1, 3) if NX == 4 else range(1, NX):
            pltpu.make_async_remote_copy(
                src_ref=out_tiles.at[r, xs[d]],
                dst_ref=turn[r].at[x],
                send_sem=turn_send.at[r],
                recv_sem=turn_recv.at[r],
                device_id=at_member(z, xs[d]),
                device_id_type=MESH,
            ).start()
        for step, base in ((1, TD + members), (groups - 1, TD + members + GG)):
            pltpu.make_async_remote_copy(
                src_ref=out_rim.at[r],
                dst_ref=ext[r].at[pl.ds(base, GG)],
                send_sem=ex_send.at[r],
                recv_sem=ex_recv.at[r],
                device_id={"group": lax.rem(g + step, groups), "member": m},
                device_id_type=MESH,
            ).start()

    moved = members - NX + 2 * GG

    def take_tiles(r):
        view = turn[r].at[pl.ds(0, NX - 1)]
        pltpu.make_async_copy(view, view, turn_recv.at[r]).wait()

        def act(pz):
            pltpu.make_async_remote_copy(
                src_ref=turn[r].at[:, pz],
                dst_ref=ext[r].at[pl.ds(TD + z * NX, NX)],
                send_sem=ex_send.at[r],
                recv_sem=ex_recv.at[r],
                device_id=at_member(pz, x),
                device_id_type=MESH,
            ).start()

        each_z(act)
        for px in range(NX):
            ext[r][TD + z * NX + px] = turn[r][px, z]
        view = ext[r].at[pl.ds(0, moved)]
        pltpu.make_async_copy(view, view, ex_recv.at[r]).wait()

        @pl.when(g == 0)
        def _():
            ext[r][TD + members : TD + members + GG] = jnp.zeros((GG, NVEC, TILE), BF16)

        @pl.when(g == groups - 1)
        def _():
            ext[r][TD + members + GG : TD + members + 2 * GG] = jnp.zeros((GG, NVEC, TILE), BF16)

    def operate(r, tiles):
        result = []
        for t in range(TD):
            picked = jnp.concatenate([ext[r][off_cols[t, k]] for k in range(K)], axis=1)
            result.append(dot(tiles[t], diag[t]) + dot(picked, off[t]))
        return result

    def push(i, src, dst, device):
        pltpu.make_async_remote_copy(
            src_ref=src,
            dst_ref=dst,
            send_sem=st_send.at[i],
            recv_sem=st_recv.at[i],
            device_id=device,
            device_id_type=MESH,
        ).start()

    def take(i, buf, count):
        view = buf.at[pl.ds(0, count)]
        pltpu.make_async_copy(view, view, st_recv.at[i]).wait()

    def send_x(i, own, buf):
        for d in range(1, NX):
            push(i, own, buf.at[x], at_member(z, xs[d]))

    def send_z(i, own, buf):
        def step(k, carry):
            push(i, own, buf.at[z], at_member(z_of(k), x))
            return carry

        lax.fori_loop(0, nz - 1, step, 0)

    def send_g(i, own, buf):
        each_group(lambda pg: push(i, own, buf.at[g], {"group": pg, "member": m}))

    def total(buf, count):
        result = buf[0]
        for j in range(1, count):
            result = result + buf[j]
        return result

    fill(0, first)

    lanes = lax.broadcasted_iota(jnp.int32, (NVEC, TILE), 1)
    packed = jnp.zeros((NVEC, TILE), F32)
    for a in range(NB // NVEC):
        rows = jnp.zeros((NVEC, TILE), F32)
        for t in range(TD):
            whole = basis[t]
            four = jnp.concatenate([whole] * (TILE // NB), axis=0)
            rows = rows + dot_nt(basis[t, NVEC * a : NVEC * (a + 1), :], four)
        packed = jnp.where(lax.div(lanes, NB) == a, rows, packed)
    packed = packed * scale_rows
    b_own[...] = packed
    bz[z] = packed
    for load in loads[2:]:
        load.wait()

    pl.semaphore_wait(barrier, nz + NX + groups - 3)
    send_tiles(0)
    take_tiles(0)

    pieces = []
    applied = operate(0, first)
    for t in range(TD):
        residual = (last[t].astype(F32) - applied[t]).astype(BF16)
        pieces.append(dot_nt(residual, prolong[t]))
    part = []
    for a in range(CTG):
        part.append(
            sum(jnp.where(agg_map[t] == a, pieces[t], jnp.zeros_like(pieces[t])) for t in range(TD))
        )
    part = jnp.concatenate(part, axis=0)
    c_own[...] = part
    cx[x] = part
    send_x(0, c_own, cx)
    send_z(3, b_own, bz)
    take(0, cx, NX - 1)
    part = total(cx, NX)
    s_own[...] = part
    cz[z] = part
    send_z(1, s_own, cz)

    take(3, bz, nz - 1)
    part = total(bz, nz)
    b2_own[...] = part
    bx[x] = part
    send_x(4, b2_own, bx)

    take(1, cz, nz - 1)
    part = total(cz, nz).astype(BF16)
    for a in range(CTG):
        g_own[a] = part[NVEC * a : NVEC * (a + 1), :]
        cg[g, a] = part[NVEC * a : NVEC * (a + 1), :]
    send_g(2, g_own, cg)

    take(4, bx, NX - 1)
    part = total(bx, NX)
    b3_own[...] = part
    bg[g] = part

    take(2, cg, groups - 1)
    coarse = jnp.concatenate([cg[c // CTG, c % CTG] for c in range(groups * CTG)], axis=1)
    correction = dot(coarse, inv[...]).astype(BF16)
    for a in range(CTG):
        corr[a] = correction[:, TILE * a : TILE * (a + 1)]
    second = []
    for t in range(TD):
        second.append((first[t].astype(F32) + dot(corr[agg_map[t]], prolong[t])).astype(BF16))
    fill(1, second)
    send_tiles(1)
    send_g(5, b3_own, bg)
    take_tiles(1)

    applied = operate(1, second)
    precond = []
    for t in range(TD):
        residual = (last[t].astype(F32) - applied[t]).astype(BF16)
        precond.append((second[t].astype(F32) + dot(residual, smooth[t])).astype(BF16))
    fill(2, precond)
    send_tiles(2)
    for t in range(TD):
        prec_ref[t] = precond[t]

    take(5, bg, groups - 1)
    packed = total(bg, groups)
    basis_total = jnp.concatenate(
        [
            packed if a == 0 else pltpu.roll(packed, TILE - NB * a, 1)
            for a in range(NB // NVEC)
        ],
        axis=0,
    )
    wide_lanes = lax.broadcasted_iota(jnp.int32, (NB, TILE), 1)
    basis_total = jnp.where(wide_lanes < NB, basis_total, 0.0)
    take_tiles(2)

    applied = [value.astype(BF16) for value in operate(2, precond)]
    part = jnp.zeros((NVEC, TILE), F32)
    for t in range(TD):
        right = jnp.concatenate(
            [basis[t], applied[t], jnp.zeros((TILE - NB - NVEC, TILE), BF16)], axis=0
        )
        part = part + dot_nt(applied[t], right)
    part = part * scale_rows
    f_own[...] = part
    fg[g] = part
    send_g(6, f_own, fg)
    take(6, fg, groups - 1)
    part = total(fg, groups)
    f2_own[...] = part
    fx[x] = part
    send_x(7, f2_own, fx)
    take(7, fx, NX - 1)
    part = total(fx, NX)
    f3_own[...] = part
    fz[z] = part
    send_z(8, f3_own, fz)
    take(8, fz, nz - 1)
    part = total(fz, nz)

    coef = jnp.where(lanes < NB, part, 0.0)
    square = pltpu.roll(part, TILE - NB, 1)
    coef_ref[...] = jnp.transpose(coef)[:NB, :]
    narrow = coef[:, :NB]
    through = exact(narrow, basis_total)
    gram = square[:, :NVEC] - 2.0 * exact_nt(coef, coef) + exact_nt(through, coef)
    gram_ref[...] = gram
    rest = [applied[t].astype(F32) - exact(narrow, basis[t].astype(F32)) for t in range(TD)]
    ids = lax.broadcasted_iota(jnp.int32, (NVEC, 1), 0)
    left = gram
    for j in range(NVEC - 1):
        pivot_row = left[j : j + 1, :]
        factor = left[:, j : j + 1] / left[j : j + 1, j : j + 1]
        factor = jnp.where(ids > j, factor, 0.0)
        left = left - factor * pivot_row
        rest = [r - factor * r[j : j + 1, :] for r in rest]
    row_ids = lax.broadcasted_iota(jnp.int32, (NVEC, NVEC), 0)
    col_ids = lax.broadcasted_iota(jnp.int32, (NVEC, NVEC), 1)
    pivots = jnp.sum(jnp.where(row_ids == col_ids, left, 0.0), axis=1, keepdims=True)
    gain = 1.0 / jnp.sqrt(pivots)
    for t in range(TD):
        new_ref[t] = rest[t] * gain

    for r in range(3):
        view = ext[r].at[pl.ds(0, moved)]
        pltpu.make_async_copy(view, view, ex_send.at[r]).wait()
        view = turn[r].at[pl.ds(0, NX - 1)]
        pltpu.make_async_copy(view, view, turn_send.at[r]).wait()
    for i, (buf, count) in enumerate(
        (
            (cx, NX), (cz, nz), (cg, groups), (bz, nz), (bx, NX), (bg, groups),
            (fg, groups), (fx, NX), (fz, nz),
        )
    ):
        view = buf.at[pl.ds(0, count - 1)]
        pltpu.make_async_copy(view, view, st_send.at[i]).wait()


def local(groups, members, off_tiles, off_cols, member_send, group_send, diag_tiles, smoother,
          agg_map, prolong, coarse_inv, krylov_basis):
    nz = members // NX
    rows_all = TD * TILE * members * groups
    hbm = pl.BlockSpec(memory_space=pl.ANY)
    smem = pl.BlockSpec(memory_space=pltpu.SMEM)
    vmem = pl.BlockSpec(memory_space=pltpu.VMEM)
    slots = TD + members + 2 * GG
    wide = (NVEC, TILE)
    call = pl.pallas_call(
        functools.partial(cycle, groups, members, rows_all),
        out_shape=(
            jax.ShapeDtypeStruct((TD, NVEC, TILE), BF16),
            jax.ShapeDtypeStruct((NB, NVEC), F32),
            jax.ShapeDtypeStruct((NVEC, NVEC), F32),
            jax.ShapeDtypeStruct((TD, NVEC, TILE), F32),
        ),
        in_specs=[smem] * 4 + [hbm] * 6,
        out_specs=(vmem,) * 4,
        scratch_shapes=[
            pltpu.VMEM((TD, K * TILE, TILE), BF16),
            pltpu.VMEM((TD, TILE, TILE), BF16),
            pltpu.VMEM((TD, TILE, TILE), BF16),
            pltpu.VMEM((TD, TILE, TILE), BF16),
            pltpu.VMEM((groups * CTG * TILE, CTG * TILE), BF16),
            pltpu.VMEM((TD, NB, TILE), BF16),
            pltpu.VMEM((3, TD, NVEC, TILE), BF16),
            pltpu.VMEM((3, NX, nz, NVEC, TILE), BF16),
            pltpu.VMEM((3, GG, NVEC, TILE), BF16),
            pltpu.VMEM((NX, nz, NVEC, TILE), BF16),
            pltpu.VMEM((NX, nz, NVEC, TILE), BF16),
            pltpu.VMEM((NX, nz, NVEC, TILE), BF16),
            pltpu.VMEM((slots, NVEC, TILE), BF16),
            pltpu.VMEM((slots, NVEC, TILE), BF16),
            pltpu.VMEM((slots, NVEC, TILE), BF16),
            pltpu.VMEM((NX, CTG * NVEC, TILE), F32),
            pltpu.VMEM((nz, CTG * NVEC, TILE), F32),
            pltpu.VMEM((groups, CTG, NVEC, TILE), BF16),
            pltpu.VMEM((CTG, NVEC, TILE), BF16),
            pltpu.VMEM((nz, *wide), F32),
            pltpu.VMEM((NX, *wide), F32),
            pltpu.VMEM((groups, *wide), F32),
            pltpu.VMEM((groups, *wide), F32),
            pltpu.VMEM((NX, *wide), F32),
            pltpu.VMEM((nz, *wide), F32),
            pltpu.VMEM((CTG * NVEC, TILE), F32),
            pltpu.VMEM((CTG * NVEC, TILE), F32),
            pltpu.VMEM((CTG, NVEC, TILE), BF16),
            pltpu.VMEM(wide, F32),
            pltpu.VMEM(wide, F32),
            pltpu.VMEM(wide, F32),
            pltpu.VMEM(wide, F32),
            pltpu.VMEM(wide, F32),
            pltpu.VMEM(wide, F32),
            pltpu.SemaphoreType.DMA((6,)),
            pltpu.SemaphoreType.DMA((3,)),
            pltpu.SemaphoreType.DMA((3,)),
            pltpu.SemaphoreType.DMA((3,)),
            pltpu.SemaphoreType.DMA((3,)),
            pltpu.SemaphoreType.DMA((9,)),
            pltpu.SemaphoreType.DMA((9,)),
        ],
        compiler_params=pltpu.CompilerParams(collective_id=0, has_side_effects=True),
        name="cycle",
    )
    return call(
        off_cols,
        member_send.reshape(members),
        group_send.reshape(GG),
        agg_map,
        off_tiles.reshape(TD, K * TILE, TILE),
        diag_tiles,
        smoother,
        prolong,
        coarse_inv,
        krylov_basis,
    )


def solution(mesh):
    groups, members = mesh.shape["group"], mesh.shape["member"]
    both = ("group", "member")
    in_specs = (
        P(both, None, None, None),
        P(both, None),
        P(both, None, None),
        P(both, None),
        P(both, None, None),
        P(both, None, None),
        P(both),
        P(both, None, None),
        P(None, "group"),
        P(both, None, None),
    )
    out_specs = (P(both, None, None), P(), P(), P(both, None, None))
    return jax.shard_map(
        functools.partial(local, groups, members),
        mesh=mesh,
        in_specs=in_specs,
        out_specs=out_specs,
        check_vma=False,
    )
```

```python
import functools

import jax
import jax.numpy as jnp
from jax import lax
from jax.experimental import pallas as pl
from jax.experimental.pallas import tpu as pltpu
from jax.sharding import PartitionSpec as P

TILE = 128
NVEC = 8
NB = 32
CTG = 2
TD = 2
K = 8
GG = 4
NX = 4
F32 = jnp.float32
BF16 = jnp.bfloat16
HIGHEST = lax.Precision.HIGHEST
MESH = pl.DeviceIdType.MESH
NT_DIMS = (((1,), (1,)), ((), ()))


def dot(left, right):
    return jnp.dot(left, right, preferred_element_type=F32)


def dot_nt(left, right):
    return lax.dot_general(left, right, NT_DIMS, preferred_element_type=F32)


def exact(left, right):
    return jnp.dot(left, right, preferred_element_type=F32, precision=HIGHEST)


def exact_nt(left, right):
    return lax.dot_general(left, right, NT_DIMS, preferred_element_type=F32, precision=HIGHEST)


def cycle(
    groups, members, rows_all,
    cols_hbm, member_hbm, rim_hbm, agg_hbm,
    off_hbm, diag_hbm, smooth_hbm, prolong_hbm, inv_hbm, basis_hbm,
    prec_ref, coef_ref, gram_ref, new_ref,
    off_cols, member_send, group_send, agg_map,
    off, diag, smooth, prolong, inv, basis,
    vals, out_tiles, out_rim, turn_0, turn_1, turn_2, ext_0, ext_1, ext_2,
    cx, cz, cg, corr,
    bz, bx, bg, fg, fx, fz,
    c_own, s_own, g_own, b_own, b2_own, b3_own, f_own, f2_own, f3_own,
    load_sem, turn_send, turn_recv, ex_send, ex_recv, st_send, st_recv,
):
    nz = members // NX
    ext = (ext_0, ext_1, ext_2)
    turn = (turn_0, turn_1, turn_2)
    g = lax.axis_index("group")
    m = lax.axis_index("member")
    z = lax.div(m, NX)
    x = lax.rem(m, NX)
    scale_rows = 1.0 / rows_all

    def at_member(pz, px):
        return {"group": g, "member": pz * NX + px}

    xs = [lax.rem(x + d, NX) for d in range(NX)]
    x_order = sorted(range(1, NX), key=lambda d: -min(d, NX - d))

    def z_of(k):
        return lax.rem(z + nz // 2 + lax.div(k + 1, 2) * (1 - 2 * lax.rem(k, 2)), nz)

    def each_z(act):
        def step(k, carry):
            act(z_of(k))
            return carry

        lax.fori_loop(0, nz - 1, step, 0)

    def each_group(act):
        def step(k, carry):
            away = lax.div(k + 1, 2) * (1 - 2 * lax.rem(k, 2))
            act(lax.rem(g + groups // 2 + away, groups))
            return carry

        lax.fori_loop(0, groups - 1, step, 0)

    barrier = pltpu.get_barrier_semaphore()
    each_z(
        lambda pz: pl.semaphore_signal(
            barrier, inc=1, device_id=at_member(pz, x), device_id_type=MESH
        )
    )
    for d in range(1, NX):
        pl.semaphore_signal(barrier, inc=1, device_id=at_member(z, xs[d]), device_id_type=MESH)
    each_group(
        lambda pg: pl.semaphore_signal(
            barrier, inc=1, device_id={"group": pg, "member": m}, device_id_type=MESH
        )
    )

    loads = [
        pltpu.make_async_copy(src, dst, load_sem.at[i])
        for i, (src, dst) in enumerate(
            (
                (basis_hbm, basis),
                (smooth_hbm, smooth),
                (off_hbm, off),
                (diag_hbm, diag),
                (prolong_hbm, prolong),
                (inv_hbm, inv),
                (member_hbm, member_send),
                (rim_hbm, group_send),
                (cols_hbm, off_cols),
                (agg_hbm, agg_map),
            )
        )
    ]
    for i in (0, 1, 6, 7, 2, 3, 8, 9, 4, 5):
        loads[i].start()

    loads[0].wait()
    loads[1].wait()
    last = [basis[t, NB - NVEC :, :] for t in range(TD)]
    first = [dot(last[t], smooth[t]).astype(BF16) for t in range(TD)]

    def fill(r, tiles):
        for t in range(TD):
            vals[r, t] = tiles[t]
            ext[r][t] = tiles[t]

        def step(pz, carry):
            for px in range(NX):
                out_tiles[r, px, pz] = vals[r, member_send[pz * NX + px]]
            turn[r][x, pz] = vals[r, member_send[pz * NX + x]]
            return carry

        lax.fori_loop(0, nz, step, 0, unroll=True)
        for s in range(GG):
            out_rim[r, s] = vals[r, group_send[s]]

    def send_tiles(r):
        for d in x_order:
            pltpu.make_async_remote_copy(
                src_ref=out_tiles.at[r, xs[d]],
                dst_ref=turn[r].at[x],
                send_sem=turn_send.at[r],
                recv_sem=turn_recv.at[r],
                device_id=at_member(z, xs[d]),
                device_id_type=MESH,
            ).start()
        for step, base in ((1, TD + members), (groups - 1, TD + members + GG)):
            pltpu.make_async_remote_copy(
                src_ref=out_rim.at[r],
                dst_ref=ext[r].at[pl.ds(base, GG)],
                send_sem=ex_send.at[r],
                recv_sem=ex_recv.at[r],
                device_id={"group": lax.rem(g + step, groups), "member": m},
                device_id_type=MESH,
            ).start()

    moved = members - NX + 2 * GG

    def take_tiles(r):
        view = turn[r].at[pl.ds(0, NX - 1)]
        pltpu.make_async_copy(view, view, turn_recv.at[r]).wait()

        def act(pz):
            pltpu.make_async_remote_copy(
                src_ref=turn[r].at[:, pz],
                dst_ref=ext[r].at[pl.ds(TD + z * NX, NX)],
                send_sem=ex_send.at[r],
                recv_sem=ex_recv.at[r],
                device_id=at_member(pz, x),
                device_id_type=MESH,
            ).start()

        each_z(act)
        for px in range(NX):
            ext[r][TD + z * NX + px] = turn[r][px, z]
        view = ext[r].at[pl.ds(0, moved)]
        pltpu.make_async_copy(view, view, ex_recv.at[r]).wait()

        @pl.when(g == 0)
        def _():
            ext[r][TD + members : TD + members + GG] = jnp.zeros((GG, NVEC, TILE), BF16)

        @pl.when(g == groups - 1)
        def _():
            ext[r][TD + members + GG : TD + members + 2 * GG] = jnp.zeros((GG, NVEC, TILE), BF16)

    def operate(r, tiles):
        result = []
        for t in range(TD):
            picked = jnp.concatenate([ext[r][off_cols[t, k]] for k in range(K)], axis=1)
            result.append(dot(tiles[t], diag[t]) + dot(picked, off[t]))
        return result

    def push(i, src, dst, device):
        pltpu.make_async_remote_copy(
            src_ref=src,
            dst_ref=dst,
            send_sem=st_send.at[i],
            recv_sem=st_recv.at[i],
            device_id=device,
            device_id_type=MESH,
        ).start()

    def take(i, buf, count):
        view = buf.at[pl.ds(0, count)]
        pltpu.make_async_copy(view, view, st_recv.at[i]).wait()

    def send_x(i, own, buf):
        for d in x_order:
            push(i, own, buf.at[x], at_member(z, xs[d]))

    def send_z(i, own, buf):
        def step(k, carry):
            push(i, own, buf.at[z], at_member(z_of(k), x))
            return carry

        lax.fori_loop(0, nz - 1, step, 0)

    def send_g(i, own, buf):
        each_group(lambda pg: push(i, own, buf.at[g], {"group": pg, "member": m}))

    def total(buf, count):
        result = buf[0]
        for j in range(1, count):
            result = result + buf[j]
        return result

    loads[6].wait()
    loads[7].wait()
    fill(0, first)

    lanes = lax.broadcasted_iota(jnp.int32, (NVEC, TILE), 1)
    packed = jnp.zeros((NVEC, TILE), F32)
    for a in range(NB // NVEC):
        rows = jnp.zeros((NVEC, TILE), F32)
        for t in range(TD):
            whole = basis[t]
            four = jnp.concatenate([whole] * (TILE // NB), axis=0)
            rows = rows + dot_nt(basis[t, NVEC * a : NVEC * (a + 1), :], four)
        packed = jnp.where(lax.div(lanes, NB) == a, rows, packed)
    packed = packed * scale_rows
    b_own[...] = packed
    bz[z] = packed
    for i in (2, 3, 4, 5, 8, 9):
        loads[i].wait()

    pl.semaphore_wait(barrier, nz + NX + groups - 3)
    send_tiles(0)
    take_tiles(0)

    pieces = []
    applied = operate(0, first)
    for t in range(TD):
        residual = (last[t].astype(F32) - applied[t]).astype(BF16)
        pieces.append(dot_nt(residual, prolong[t]))
    part = []
    for a in range(CTG):
        part.append(
            sum(jnp.where(agg_map[t] == a, pieces[t], jnp.zeros_like(pieces[t])) for t in range(TD))
        )
    part = jnp.concatenate(part, axis=0)
    c_own[...] = part
    cx[x] = part
    send_x(0, c_own, cx)
    take(0, cx, NX - 1)
    part = total(cx, NX)
    s_own[...] = part
    cz[z] = part
    send_z(1, s_own, cz)

    take(1, cz, nz - 1)
    part = total(cz, nz).astype(BF16)
    for a in range(CTG):
        g_own[a] = part[NVEC * a : NVEC * (a + 1), :]
        cg[g, a] = part[NVEC * a : NVEC * (a + 1), :]
    send_g(2, g_own, cg)
    send_z(3, b_own, bz)

    take(2, cg, groups - 1)
    coarse = jnp.concatenate([cg[c // CTG, c % CTG] for c in range(groups * CTG)], axis=1)
    correction = dot(coarse, inv[...]).astype(BF16)
    for a in range(CTG):
        corr[a] = correction[:, TILE * a : TILE * (a + 1)]
    second = []
    for t in range(TD):
        second.append((first[t].astype(F32) + dot(corr[agg_map[t]], prolong[t])).astype(BF16))
    fill(1, second)
    send_tiles(1)
    take(3, bz, nz - 1)
    part = total(bz, nz)
    b2_own[...] = part
    bx[x] = part
    send_x(4, b2_own, bx)
    take_tiles(1)

    applied = operate(1, second)
    precond = []
    for t in range(TD):
        residual = (last[t].astype(F32) - applied[t]).astype(BF16)
        precond.append((second[t].astype(F32) + dot(residual, smooth[t])).astype(BF16))
    fill(2, precond)
    send_tiles(2)
    for t in range(TD):
        prec_ref[t] = precond[t]

    take(4, bx, NX - 1)
    part = total(bx, NX)
    b3_own[...] = part
    bg[g] = part
    send_g(5, b3_own, bg)
    take_tiles(2)

    applied = [value.astype(BF16) for value in operate(2, precond)]
    part = jnp.zeros((NVEC, TILE), F32)
    for t in range(TD):
        right = jnp.concatenate(
            [basis[t], applied[t], jnp.zeros((TILE - NB - NVEC, TILE), BF16)], axis=0
        )
        part = part + dot_nt(applied[t], right)
    part = part * scale_rows
    f_own[...] = part
    fg[g] = part
    send_g(6, f_own, fg)
    take(6, fg, groups - 1)
    part = total(fg, groups)
    f2_own[...] = part
    fx[x] = part
    send_x(7, f2_own, fx)
    take(7, fx, NX - 1)
    part = total(fx, NX)
    f3_own[...] = part
    fz[z] = part
    send_z(8, f3_own, fz)
    take(5, bg, groups - 1)
    packed = total(bg, groups)
    basis_total = jnp.concatenate(
        [
            packed if a == 0 else pltpu.roll(packed, TILE - NB * a, 1)
            for a in range(NB // NVEC)
        ],
        axis=0,
    )
    wide_lanes = lax.broadcasted_iota(jnp.int32, (NB, TILE), 1)
    wide_rows = lax.broadcasted_iota(jnp.int32, (NB, TILE), 0)
    basis_total = jnp.where(wide_lanes < NB, basis_total, 0.0)
    mirror = jnp.where(wide_rows == wide_lanes, 2.0, 0.0) - basis_total
    take(8, fz, nz - 1)
    part = total(fz, nz)

    coef = jnp.where(lanes < NB, part, 0.0)
    square = pltpu.roll(part, TILE - NB, 1)
    coef_ref[...] = part[:, :NB]
    narrow = coef[:, :NB]
    gram = square[:, :NVEC] - exact_nt(exact(narrow, mirror), coef)
    gram_ref[...] = gram
    rest = [applied[t].astype(F32) - exact(narrow, basis[t].astype(F32)) for t in range(TD)]
    ids = lax.broadcasted_iota(jnp.int32, (NVEC, 1), 0)
    left = gram
    for j in range(NVEC - 1):
        pivot_row = left[j : j + 1, :]
        factor = left[:, j : j + 1] / left[j : j + 1, j : j + 1]
        factor = jnp.where(ids > j, factor, 0.0)
        left = left - factor * pivot_row
        rest = [r - factor * r[j : j + 1, :] for r in rest]
    row_ids = lax.broadcasted_iota(jnp.int32, (NVEC, NVEC), 0)
    col_ids = lax.broadcasted_iota(jnp.int32, (NVEC, NVEC), 1)
    pivots = jnp.sum(jnp.where(row_ids == col_ids, left, 0.0), axis=1, keepdims=True)
    gain = 1.0 / jnp.sqrt(pivots)
    for t in range(TD):
        new_ref[t] = rest[t] * gain

    for r in range(3):
        view = ext[r].at[pl.ds(0, moved)]
        pltpu.make_async_copy(view, view, ex_send.at[r]).wait()
        view = turn[r].at[pl.ds(0, NX - 1)]
        pltpu.make_async_copy(view, view, turn_send.at[r]).wait()
    for i, (buf, count) in enumerate(
        (
            (cx, NX), (cz, nz), (cg, groups), (bz, nz), (bx, NX), (bg, groups),
            (fg, groups), (fx, NX), (fz, nz),
        )
    ):
        view = buf.at[pl.ds(0, count - 1)]
        pltpu.make_async_copy(view, view, st_send.at[i]).wait()


def finish(*refs):
    sem = refs[8]
    copies = [pltpu.make_async_copy(refs[i], refs[4 + i], sem.at[i]) for i in range(4)]
    for copy in copies:
        copy.start()
    for copy in copies:
        copy.wait()


def local(groups, members, off_tiles, off_cols, member_send, group_send, diag_tiles, smoother,
          agg_map, prolong, coarse_inv, krylov_basis):
    nz = members // NX
    rows_all = TD * TILE * members * groups
    hbm = pl.BlockSpec(memory_space=pltpu.HBM)
    vmem = pl.BlockSpec(memory_space=pltpu.VMEM)
    slots = TD + members + 2 * GG
    wide = (NVEC, TILE)
    call = pl.pallas_call(
        functools.partial(cycle, groups, members, rows_all),
        out_shape=(
            jax.ShapeDtypeStruct((TD, NVEC, TILE), BF16),
            jax.ShapeDtypeStruct((NVEC, NB), F32),
            jax.ShapeDtypeStruct((NVEC, NVEC), F32),
            jax.ShapeDtypeStruct((TD, NVEC, TILE), F32),
        ),
        in_specs=[hbm] * 10,
        out_specs=(vmem,) * 4,
        scratch_shapes=[
            pltpu.SMEM((TD, K), jnp.int32),
            pltpu.SMEM((members,), jnp.int32),
            pltpu.SMEM((GG,), jnp.int32),
            pltpu.SMEM((TD,), jnp.int32),
            pltpu.VMEM((TD, K * TILE, TILE), BF16),
            pltpu.VMEM((TD, TILE, TILE), BF16),
            pltpu.VMEM((TD, TILE, TILE), BF16),
            pltpu.VMEM((TD, TILE, TILE), BF16),
            pltpu.VMEM((groups * CTG * TILE, CTG * TILE), BF16),
            pltpu.VMEM((TD, NB, TILE), BF16),
            pltpu.VMEM((3, TD, NVEC, TILE), BF16),
            pltpu.VMEM((3, NX, nz, NVEC, TILE), BF16),
            pltpu.VMEM((3, GG, NVEC, TILE), BF16),
            pltpu.VMEM((NX, nz, NVEC, TILE), BF16),
            pltpu.VMEM((NX, nz, NVEC, TILE), BF16),
            pltpu.VMEM((NX, nz, NVEC, TILE), BF16),
            pltpu.VMEM((slots, NVEC, TILE), BF16),
            pltpu.VMEM((slots, NVEC, TILE), BF16),
            pltpu.VMEM((slots, NVEC, TILE), BF16),
            pltpu.VMEM((NX, CTG * NVEC, TILE), F32),
            pltpu.VMEM((nz, CTG * NVEC, TILE), F32),
            pltpu.VMEM((groups, CTG, NVEC, TILE), BF16),
            pltpu.VMEM((CTG, NVEC, TILE), BF16),
            pltpu.VMEM((nz, *wide), F32),
            pltpu.VMEM((NX, *wide), F32),
            pltpu.VMEM((groups, *wide), F32),
            pltpu.VMEM((groups, *wide), F32),
            pltpu.VMEM((NX, *wide), F32),
            pltpu.VMEM((nz, *wide), F32),
            pltpu.VMEM((CTG * NVEC, TILE), F32),
            pltpu.VMEM((CTG * NVEC, TILE), F32),
            pltpu.VMEM((CTG, NVEC, TILE), BF16),
            pltpu.VMEM(wide, F32),
            pltpu.VMEM(wide, F32),
            pltpu.VMEM(wide, F32),
            pltpu.VMEM(wide, F32),
            pltpu.VMEM(wide, F32),
            pltpu.VMEM(wide, F32),
            pltpu.SemaphoreType.DMA((10,)),
            pltpu.SemaphoreType.DMA((3,)),
            pltpu.SemaphoreType.DMA((3,)),
            pltpu.SemaphoreType.DMA((3,)),
            pltpu.SemaphoreType.DMA((3,)),
            pltpu.SemaphoreType.DMA((9,)),
            pltpu.SemaphoreType.DMA((9,)),
        ],
        compiler_params=pltpu.CompilerParams(
            collective_id=0, has_side_effects=True, vmem_limit_bytes=16 << 20
        ),
        name="cycle",
    )
    arrays = (
        off_cols,
        member_send.reshape(members),
        group_send.reshape(GG),
        agg_map,
        off_tiles.reshape(TD, K * TILE, TILE),
        diag_tiles,
        smoother,
        prolong,
        coarse_inv,
        krylov_basis,
    )
    results = call(*(pltpu.with_memory_space_constraint(v, pltpu.HBM) for v in arrays))
    hand_out = pl.pallas_call(
        finish,
        out_shape=tuple(jax.ShapeDtypeStruct(r.shape, r.dtype) for r in results),
        in_specs=[vmem] * 4,
        out_specs=(hbm,) * 4,
        scratch_shapes=[pltpu.SemaphoreType.DMA((4,))],
        compiler_params=pltpu.CompilerParams(vmem_limit_bytes=1 << 20),
        name="finish",
    )
    precond, coef, gram, new_block = hand_out(*results)
    return precond, coef.T, gram, new_block


def solution(mesh):
    groups, members = mesh.shape["group"], mesh.shape["member"]
    both = ("group", "member")
    in_specs = (
        P(both, None, None, None),
        P(both, None),
        P(both, None, None),
        P(both, None),
        P(both, None, None),
        P(both, None, None),
        P(both),
        P(both, None, None),
        P(None, "group"),
        P(both, None, None),
    )
    out_specs = (P(both, None, None), P(), P(), P(both, None, None))
    return jax.shard_map(
        functools.partial(local, groups, members),
        mesh=mesh,
        in_specs=in_specs,
        out_specs=out_specs,
        check_vma=False,
    )
```

```python
import functools

import jax
import jax.numpy as jnp
from jax import lax
from jax.experimental import pallas as pl
from jax.experimental.pallas import tpu as pltpu
from jax.sharding import PartitionSpec as P

TILE = 128
NVEC = 8
NB = 32
CTG = 2
TD = 2
K = 8
GG = 4
NX = 4
NF = 5
F32 = jnp.float32
BF16 = jnp.bfloat16
HIGHEST = lax.Precision.HIGHEST
MESH = pl.DeviceIdType.MESH
NT_DIMS = (((1,), (1,)), ((), ()))


def dot(left, right):
    return jnp.dot(left, right, preferred_element_type=F32)


def dot_nt(left, right):
    return lax.dot_general(left, right, NT_DIMS, preferred_element_type=F32)


def exact(left, right):
    return jnp.dot(left, right, preferred_element_type=F32, precision=HIGHEST)


def exact_nt(left, right):
    return lax.dot_general(left, right, NT_DIMS, preferred_element_type=F32, precision=HIGHEST)


def cycle(
    groups, members, rows_all,
    cols_hbm, member_hbm, rim_hbm, agg_hbm,
    off_hbm, diag_hbm, smooth_hbm, prolong_hbm, inv_hbm, basis_hbm,
    prec_ref, coef_ref, gram_ref, new_ref,
    off_cols, member_send, group_send, agg_map,
    off, diag, smooth, prolong, inv, basis,
    vals, far_tiles, out_tiles, out_rim, turn_0, turn_1, turn_2, ext_0, ext_1, ext_2,
    cx, cz, cg, corr,
    bz, bx, bg, fg, fx, fz,
    c_own, s_own, g_own, b_own, b2_own, b3_own, f_own, f2_own, f3_own,
    load_sem, turn_send, turn_recv, ex_send, ex_recv, st_send, st_recv,
):
    nz = members // NX
    ext = (ext_0, ext_1, ext_2)
    turn = (turn_0, turn_1, turn_2)
    g = lax.axis_index("group")
    m = lax.axis_index("member")
    z = lax.div(m, NX)
    x = lax.rem(m, NX)
    scale_rows = 1.0 / rows_all

    def away(k):
        return nz // 2 + (k + 1) // 2 * (1 - 2 * (k % 2))

    near = [*(away(k) for k in range(NF, nz - 1)), 0]

    def at_member(pz, px):
        return {"group": g, "member": pz * NX + px}

    xs = [lax.rem(x + d, NX) for d in range(NX)]
    x_order = sorted(range(1, NX), key=lambda d: -min(d, NX - d))

    def z_of(k):
        return lax.rem(z + nz // 2 + lax.div(k + 1, 2) * (1 - 2 * lax.rem(k, 2)), nz)

    def each_far(act):
        def step(k, carry):
            pz = z_of(k)
            for px in range(NX):
                act(k, pz, px)
            return carry

        lax.fori_loop(0, NF, step, 0)

    def each_z(act):
        def step(k, carry):
            act(z_of(k))
            return carry

        lax.fori_loop(0, nz - 1, step, 0)

    def each_group(act):
        def step(k, carry):
            away = lax.div(k + 1, 2) * (1 - 2 * lax.rem(k, 2))
            act(lax.rem(g + groups // 2 + away, groups))
            return carry

        lax.fori_loop(0, groups - 1, step, 0)

    barrier = pltpu.get_barrier_semaphore()
    each_far(
        lambda k, pz, px: pl.semaphore_signal(
            barrier, inc=1, device_id=at_member(pz, px), device_id_type=MESH
        )
    )
    for dz in near[:-1]:
        pl.semaphore_signal(
            barrier, inc=1, device_id=at_member(lax.rem(z + dz, nz), x), device_id_type=MESH
        )
    for d in range(1, NX):
        pl.semaphore_signal(barrier, inc=1, device_id=at_member(z, xs[d]), device_id_type=MESH)
    each_group(
        lambda pg: pl.semaphore_signal(
            barrier, inc=1, device_id={"group": pg, "member": m}, device_id_type=MESH
        )
    )

    loads = [
        pltpu.make_async_copy(src, dst, load_sem.at[i])
        for i, (src, dst) in enumerate(
            (
                (basis_hbm, basis),
                (smooth_hbm, smooth),
                (off_hbm, off),
                (diag_hbm, diag),
                (prolong_hbm, prolong),
                (inv_hbm, inv),
                (member_hbm, member_send),
                (rim_hbm, group_send),
                (cols_hbm, off_cols),
                (agg_hbm, agg_map),
            )
        )
    ]
    for i in (0, 1, 6, 7, 2, 3, 8, 9, 4, 5):
        loads[i].start()

    loads[0].wait()
    loads[1].wait()
    last = [basis[t, NB - NVEC :, :] for t in range(TD)]
    first = [dot(last[t], smooth[t]).astype(BF16) for t in range(TD)]

    def fill(r, tiles):
        for t in range(TD):
            vals[r, t] = tiles[t]
            ext[r][t] = tiles[t]

        for k in range(NF):
            pz = lax.rem(z + away(k), nz)
            for px in range(NX):
                far_tiles[r, k, px] = vals[r, member_send[pz * NX + px]]
        for j, dz in enumerate(near):
            pz = lax.rem(z + dz, nz)
            for px in range(NX):
                out_tiles[r, px, j] = vals[r, member_send[pz * NX + px]]
            turn[r][x, j] = vals[r, member_send[pz * NX + x]]
        for s in range(GG):
            out_rim[r, s] = vals[r, group_send[s]]

    def send_tiles(r):
        each_far(
            lambda k, pz, px: pltpu.make_async_remote_copy(
                src_ref=far_tiles.at[r, k, px],
                dst_ref=ext[r].at[TD + m],
                send_sem=ex_send.at[r],
                recv_sem=ex_recv.at[r],
                device_id=at_member(pz, px),
                device_id_type=MESH,
            ).start()
        )
        for d in x_order:
            pltpu.make_async_remote_copy(
                src_ref=out_tiles.at[r, xs[d]],
                dst_ref=turn[r].at[x],
                send_sem=turn_send.at[r],
                recv_sem=turn_recv.at[r],
                device_id=at_member(z, xs[d]),
                device_id_type=MESH,
            ).start()
        for step, base in ((1, TD + members), (groups - 1, TD + members + GG)):
            pltpu.make_async_remote_copy(
                src_ref=out_rim.at[r],
                dst_ref=ext[r].at[pl.ds(base, GG)],
                send_sem=ex_send.at[r],
                recv_sem=ex_recv.at[r],
                device_id={"group": lax.rem(g + step, groups), "member": m},
                device_id_type=MESH,
            ).start()

    moved = members - NX + 2 * GG

    def take_tiles(r):
        view = turn[r].at[pl.ds(0, NX - 1)]
        pltpu.make_async_copy(view, view, turn_recv.at[r]).wait()

        for j, dz in enumerate(near[:-1]):
            pltpu.make_async_remote_copy(
                src_ref=turn[r].at[:, j],
                dst_ref=ext[r].at[pl.ds(TD + z * NX, NX)],
                send_sem=ex_send.at[r],
                recv_sem=ex_recv.at[r],
                device_id=at_member(lax.rem(z + dz, nz), x),
                device_id_type=MESH,
            ).start()
        for px in range(NX):
            ext[r][TD + z * NX + px] = turn[r][px, len(near) - 1]
        view = ext[r].at[pl.ds(0, moved)]
        pltpu.make_async_copy(view, view, ex_recv.at[r]).wait()

        @pl.when(g == 0)
        def _():
            ext[r][TD + members : TD + members + GG] = jnp.zeros((GG, NVEC, TILE), BF16)

        @pl.when(g == groups - 1)
        def _():
            ext[r][TD + members + GG : TD + members + 2 * GG] = jnp.zeros((GG, NVEC, TILE), BF16)

    def operate(r, tiles):
        result = []
        for t in range(TD):
            picked = jnp.concatenate([ext[r][off_cols[t, k]] for k in range(K)], axis=1)
            result.append(dot(tiles[t], diag[t]) + dot(picked, off[t]))
        return result

    def push(i, src, dst, device):
        pltpu.make_async_remote_copy(
            src_ref=src,
            dst_ref=dst,
            send_sem=st_send.at[i],
            recv_sem=st_recv.at[i],
            device_id=device,
            device_id_type=MESH,
        ).start()

    def take(i, buf, count):
        view = buf.at[pl.ds(0, count)]
        pltpu.make_async_copy(view, view, st_recv.at[i]).wait()

    def send_x(i, own, buf):
        for d in x_order:
            push(i, own, buf.at[x], at_member(z, xs[d]))

    def send_z(i, own, buf):
        def step(k, carry):
            push(i, own, buf.at[z], at_member(z_of(k), x))
            return carry

        lax.fori_loop(0, nz - 1, step, 0)

    def send_g(i, own, buf):
        each_group(lambda pg: push(i, own, buf.at[g], {"group": pg, "member": m}))

    def total(buf, count):
        result = buf[0]
        for j in range(1, count):
            result = result + buf[j]
        return result

    loads[6].wait()
    loads[7].wait()
    fill(0, first)

    lanes = lax.broadcasted_iota(jnp.int32, (NVEC, TILE), 1)
    packed = jnp.zeros((NVEC, TILE), F32)
    for a in range(NB // NVEC):
        rows = jnp.zeros((NVEC, TILE), F32)
        for t in range(TD):
            whole = basis[t]
            four = jnp.concatenate([whole] * (TILE // NB), axis=0)
            rows = rows + dot_nt(basis[t, NVEC * a : NVEC * (a + 1), :], four)
        packed = jnp.where(lax.div(lanes, NB) == a, rows, packed)
    packed = packed * scale_rows
    b_own[...] = packed
    bz[z] = packed
    for i in (2, 3, 4, 5, 8, 9):
        loads[i].wait()

    pl.semaphore_wait(barrier, NF * NX + len(near) + NX + groups - 3)
    send_tiles(0)
    take_tiles(0)

    pieces = []
    applied = operate(0, first)
    for t in range(TD):
        residual = (last[t].astype(F32) - applied[t]).astype(BF16)
        pieces.append(dot_nt(residual, prolong[t]))
    part = []
    for a in range(CTG):
        part.append(
            sum(jnp.where(agg_map[t] == a, pieces[t], jnp.zeros_like(pieces[t])) for t in range(TD))
        )
    part = jnp.concatenate(part, axis=0)
    c_own[...] = part
    cx[x] = part
    send_x(0, c_own, cx)
    take(0, cx, NX - 1)
    part = total(cx, NX)
    s_own[...] = part
    cz[z] = part
    send_z(1, s_own, cz)

    take(1, cz, nz - 1)
    part = total(cz, nz).astype(BF16)
    for a in range(CTG):
        g_own[a] = part[NVEC * a : NVEC * (a + 1), :]
        cg[g, a] = part[NVEC * a : NVEC * (a + 1), :]
    send_g(2, g_own, cg)
    send_z(3, b_own, bz)

    take(2, cg, groups - 1)
    coarse = jnp.concatenate([cg[c // CTG, c % CTG] for c in range(groups * CTG)], axis=1)
    correction = dot(coarse, inv[...]).astype(BF16)
    for a in range(CTG):
        corr[a] = correction[:, TILE * a : TILE * (a + 1)]
    second = []
    for t in range(TD):
        second.append((first[t].astype(F32) + dot(corr[agg_map[t]], prolong[t])).astype(BF16))
    fill(1, second)
    send_tiles(1)
    take(3, bz, nz - 1)
    part = total(bz, nz)
    b2_own[...] = part
    bx[x] = part
    send_x(4, b2_own, bx)
    take_tiles(1)

    applied = operate(1, second)
    precond = []
    for t in range(TD):
        residual = (last[t].astype(F32) - applied[t]).astype(BF16)
        precond.append((second[t].astype(F32) + dot(residual, smooth[t])).astype(BF16))
    fill(2, precond)
    send_tiles(2)
    for t in range(TD):
        prec_ref[t] = precond[t]

    take(4, bx, NX - 1)
    part = total(bx, NX)
    b3_own[...] = part
    bg[g] = part
    send_g(5, b3_own, bg)
    take_tiles(2)

    applied = [value.astype(BF16) for value in operate(2, precond)]
    part = jnp.zeros((NVEC, TILE), F32)
    for t in range(TD):
        right = jnp.concatenate(
            [basis[t], applied[t], jnp.zeros((TILE - NB - NVEC, TILE), BF16)], axis=0
        )
        part = part + dot_nt(applied[t], right)
    part = part * scale_rows
    f_own[...] = part
    fg[g] = part
    send_g(6, f_own, fg)
    take(6, fg, groups - 1)
    part = total(fg, groups)
    f2_own[...] = part
    fx[x] = part
    send_x(7, f2_own, fx)
    take(7, fx, NX - 1)
    part = total(fx, NX)
    f3_own[...] = part
    fz[z] = part
    send_z(8, f3_own, fz)
    take(5, bg, groups - 1)
    packed = total(bg, groups)
    basis_total = jnp.concatenate(
        [
            packed if a == 0 else pltpu.roll(packed, TILE - NB * a, 1)
            for a in range(NB // NVEC)
        ],
        axis=0,
    )
    wide_lanes = lax.broadcasted_iota(jnp.int32, (NB, TILE), 1)
    wide_rows = lax.broadcasted_iota(jnp.int32, (NB, TILE), 0)
    basis_total = jnp.where(wide_lanes < NB, basis_total, 0.0)
    mirror = jnp.where(wide_rows == wide_lanes, 2.0, 0.0) - basis_total
    take(8, fz, nz - 1)
    part = total(fz, nz)

    coef = jnp.where(lanes < NB, part, 0.0)
    square = pltpu.roll(part, TILE - NB, 1)
    coef_ref[...] = part[:, :NB]
    narrow = coef[:, :NB]
    gram = square[:, :NVEC] - exact_nt(exact(narrow, mirror), coef)
    gram_ref[...] = gram
    rest = [applied[t].astype(F32) - exact(narrow, basis[t].astype(F32)) for t in range(TD)]
    ids = lax.broadcasted_iota(jnp.int32, (NVEC, 1), 0)
    left = gram
    for j in range(NVEC - 1):
        pivot_row = left[j : j + 1, :]
        factor = left[:, j : j + 1] / left[j : j + 1, j : j + 1]
        factor = jnp.where(ids > j, factor, 0.0)
        left = left - factor * pivot_row
        rest = [r - factor * r[j : j + 1, :] for r in rest]
    row_ids = lax.broadcasted_iota(jnp.int32, (NVEC, NVEC), 0)
    col_ids = lax.broadcasted_iota(jnp.int32, (NVEC, NVEC), 1)
    pivots = jnp.sum(jnp.where(row_ids == col_ids, left, 0.0), axis=1, keepdims=True)
    gain = 1.0 / jnp.sqrt(pivots)
    for t in range(TD):
        new_ref[t] = rest[t] * gain

    for r in range(3):
        view = ext[r].at[pl.ds(0, moved)]
        pltpu.make_async_copy(view, view, ex_send.at[r]).wait()
        view = turn[r].at[pl.ds(0, NX - 1)]
        pltpu.make_async_copy(view, view, turn_send.at[r]).wait()
    for i, (buf, count) in enumerate(
        (
            (cx, NX), (cz, nz), (cg, groups), (bz, nz), (bx, NX), (bg, groups),
            (fg, groups), (fx, NX), (fz, nz),
        )
    ):
        view = buf.at[pl.ds(0, count - 1)]
        pltpu.make_async_copy(view, view, st_send.at[i]).wait()


def finish(*refs):
    sem = refs[8]
    copies = [pltpu.make_async_copy(refs[i], refs[4 + i], sem.at[i]) for i in range(4)]
    for copy in copies:
        copy.start()
    for copy in copies:
        copy.wait()


def local(groups, members, off_tiles, off_cols, member_send, group_send, diag_tiles, smoother,
          agg_map, prolong, coarse_inv, krylov_basis):
    nz = members // NX
    rows_all = TD * TILE * members * groups
    hbm = pl.BlockSpec(memory_space=pltpu.HBM)
    vmem = pl.BlockSpec(memory_space=pltpu.VMEM)
    slots = TD + members + 2 * GG
    wide = (NVEC, TILE)
    call = pl.pallas_call(
        functools.partial(cycle, groups, members, rows_all),
        out_shape=(
            jax.ShapeDtypeStruct((TD, NVEC, TILE), BF16),
            jax.ShapeDtypeStruct((NVEC, NB), F32),
            jax.ShapeDtypeStruct((NVEC, NVEC), F32),
            jax.ShapeDtypeStruct((TD, NVEC, TILE), F32),
        ),
        in_specs=[hbm] * 10,
        out_specs=(vmem,) * 4,
        scratch_shapes=[
            pltpu.SMEM((TD, K), jnp.int32),
            pltpu.SMEM((members,), jnp.int32),
            pltpu.SMEM((GG,), jnp.int32),
            pltpu.SMEM((TD,), jnp.int32),
            pltpu.VMEM((TD, K * TILE, TILE), BF16),
            pltpu.VMEM((TD, TILE, TILE), BF16),
            pltpu.VMEM((TD, TILE, TILE), BF16),
            pltpu.VMEM((TD, TILE, TILE), BF16),
            pltpu.VMEM((groups * CTG * TILE, CTG * TILE), BF16),
            pltpu.VMEM((TD, NB, TILE), BF16),
            pltpu.VMEM((3, TD, NVEC, TILE), BF16),
            pltpu.VMEM((3, NF, NX, NVEC, TILE), BF16),
            pltpu.VMEM((3, NX, nz - NF, NVEC, TILE), BF16),
            pltpu.VMEM((3, GG, NVEC, TILE), BF16),
            pltpu.VMEM((NX, nz - NF, NVEC, TILE), BF16),
            pltpu.VMEM((NX, nz - NF, NVEC, TILE), BF16),
            pltpu.VMEM((NX, nz - NF, NVEC, TILE), BF16),
            pltpu.VMEM((slots, NVEC, TILE), BF16),
            pltpu.VMEM((slots, NVEC, TILE), BF16),
            pltpu.VMEM((slots, NVEC, TILE), BF16),
            pltpu.VMEM((NX, CTG * NVEC, TILE), F32),
            pltpu.VMEM((nz, CTG * NVEC, TILE), F32),
            pltpu.VMEM((groups, CTG, NVEC, TILE), BF16),
            pltpu.VMEM((CTG, NVEC, TILE), BF16),
            pltpu.VMEM((nz, *wide), F32),
            pltpu.VMEM((NX, *wide), F32),
            pltpu.VMEM((groups, *wide), F32),
            pltpu.VMEM((groups, *wide), F32),
            pltpu.VMEM((NX, *wide), F32),
            pltpu.VMEM((nz, *wide), F32),
            pltpu.VMEM((CTG * NVEC, TILE), F32),
            pltpu.VMEM((CTG * NVEC, TILE), F32),
            pltpu.VMEM((CTG, NVEC, TILE), BF16),
            pltpu.VMEM(wide, F32),
            pltpu.VMEM(wide, F32),
            pltpu.VMEM(wide, F32),
            pltpu.VMEM(wide, F32),
            pltpu.VMEM(wide, F32),
            pltpu.VMEM(wide, F32),
            pltpu.SemaphoreType.DMA((10,)),
            pltpu.SemaphoreType.DMA((3,)),
            pltpu.SemaphoreType.DMA((3,)),
            pltpu.SemaphoreType.DMA((3,)),
            pltpu.SemaphoreType.DMA((3,)),
            pltpu.SemaphoreType.DMA((9,)),
            pltpu.SemaphoreType.DMA((9,)),
        ],
        compiler_params=pltpu.CompilerParams(
            collective_id=0, has_side_effects=True, vmem_limit_bytes=16 << 20
        ),
        name="cycle",
    )
    arrays = (
        off_cols,
        member_send.reshape(members),
        group_send.reshape(GG),
        agg_map,
        off_tiles.reshape(TD, K * TILE, TILE),
        diag_tiles,
        smoother,
        prolong,
        coarse_inv,
        krylov_basis,
    )
    results = call(*(pltpu.with_memory_space_constraint(v, pltpu.HBM) for v in arrays))
    hand_out = pl.pallas_call(
        finish,
        out_shape=tuple(jax.ShapeDtypeStruct(r.shape, r.dtype) for r in results),
        in_specs=[vmem] * 4,
        out_specs=(hbm,) * 4,
        scratch_shapes=[pltpu.SemaphoreType.DMA((4,))],
        compiler_params=pltpu.CompilerParams(vmem_limit_bytes=1 << 20),
        name="finish",
    )
    precond, coef, gram, new_block = hand_out(*results)
    return precond, coef.T, gram, new_block


def solution(mesh):
    groups, members = mesh.shape["group"], mesh.shape["member"]
    both = ("group", "member")
    in_specs = (
        P(both, None, None, None),
        P(both, None),
        P(both, None, None),
        P(both, None),
        P(both, None, None),
        P(both, None, None),
        P(both),
        P(both, None, None),
        P(None, "group"),
        P(both, None, None),
    )
    out_specs = (P(both, None, None), P(), P(), P(both, None, None))
    return jax.shard_map(
        functools.partial(local, groups, members),
        mesh=mesh,
        in_specs=in_specs,
        out_specs=out_specs,
        check_vma=False,
    )
```

```python
import functools

import jax
import jax.numpy as jnp
from jax import lax
from jax.experimental import pallas as pl
from jax.experimental.pallas import tpu as pltpu
from jax.sharding import PartitionSpec as P

TILE = 128
NVEC = 8
NB = 32
CTG = 2
TD = 2
K = 8
GG = 4
NX = 4
NF = 5
F32 = jnp.float32
BF16 = jnp.bfloat16
HIGHEST = lax.Precision.HIGHEST
MESH = pl.DeviceIdType.MESH
NT_DIMS = (((1,), (1,)), ((), ()))


def dot(left, right):
    return jnp.dot(left, right, preferred_element_type=F32)


def dot_nt(left, right):
    return lax.dot_general(left, right, NT_DIMS, preferred_element_type=F32)


def exact(left, right):
    return jnp.dot(left, right, preferred_element_type=F32, precision=HIGHEST)


def exact_nt(left, right):
    return lax.dot_general(left, right, NT_DIMS, preferred_element_type=F32, precision=HIGHEST)


def cycle(
    groups, members, rows_all,
    cols_hbm, member_hbm, rim_hbm, agg_hbm,
    off_hbm, diag_hbm, smooth_hbm, prolong_hbm, inv_hbm, basis_hbm,
    prec_ref, coef_ref, gram_ref, new_ref,
    off_cols, member_send, group_send, agg_map,
    off, diag, smooth, prolong, inv, basis,
    vals, far_tiles, out_tiles, out_rim, turn_0, turn_1, turn_2, ext_0, ext_1, ext_2,
    cx, cz, cg, corr,
    bz, bx, bg, fg, fx, ff, fz, fold,
    c_own, s_own, g_own, b_own, b2_own, b3_own, f_own, f2_own, f3_own,
    load_sem, turn_send, turn_recv, ex_send, ex_recv, st_send, st_recv,
):
    nz = members // NX
    ext = (ext_0, ext_1, ext_2)
    turn = (turn_0, turn_1, turn_2)
    g = lax.axis_index("group")
    m = lax.axis_index("member")
    z = lax.div(m, NX)
    x = lax.rem(m, NX)
    scale_rows = 1.0 / rows_all

    def away(k):
        return nz // 2 + (k + 1) // 2 * (1 - 2 * (k % 2))

    near = [*(away(k) for k in range(NF, nz - 1)), 0]

    def at_member(pz, px):
        return {"group": g, "member": pz * NX + px}

    xs = [lax.rem(x + d, NX) for d in range(NX)]
    x_order = sorted(range(1, NX), key=lambda d: -min(d, NX - d))

    def z_of(k):
        return lax.rem(z + nz // 2 + lax.div(k + 1, 2) * (1 - 2 * lax.rem(k, 2)), nz)

    def each_far(act):
        def step(k, carry):
            pz = z_of(k)
            for px in range(NX):
                act(k, pz, px)
            return carry

        lax.fori_loop(0, NF, step, 0)

    def each_z(act):
        def step(k, carry):
            act(z_of(k))
            return carry

        lax.fori_loop(0, nz - 1, step, 0)

    def each_group(act):
        def step(k, carry):
            away = lax.div(k + 1, 2) * (1 - 2 * lax.rem(k, 2))
            act(lax.rem(g + groups // 2 + away, groups))
            return carry

        lax.fori_loop(0, groups - 1, step, 0)

    barrier = pltpu.get_barrier_semaphore()
    each_far(
        lambda k, pz, px: pl.semaphore_signal(
            barrier, inc=1, device_id=at_member(pz, px), device_id_type=MESH
        )
    )
    for dz in near[:-1]:
        pl.semaphore_signal(
            barrier, inc=1, device_id=at_member(lax.rem(z + dz, nz), x), device_id_type=MESH
        )
    for d in range(1, NX):
        pl.semaphore_signal(barrier, inc=1, device_id=at_member(z, xs[d]), device_id_type=MESH)
    each_group(
        lambda pg: pl.semaphore_signal(
            barrier, inc=1, device_id={"group": pg, "member": m}, device_id_type=MESH
        )
    )

    loads = [
        pltpu.make_async_copy(src, dst, load_sem.at[i])
        for i, (src, dst) in enumerate(
            (
                (basis_hbm, basis),
                (smooth_hbm, smooth),
                (off_hbm, off),
                (diag_hbm, diag),
                (prolong_hbm, prolong),
                (inv_hbm, inv),
                (member_hbm, member_send),
                (rim_hbm, group_send),
                (cols_hbm, off_cols),
                (agg_hbm, agg_map),
            )
        )
    ]
    for i in (0, 1, 6, 7, 2, 3, 8, 9, 4, 5):
        loads[i].start()

    loads[0].wait()
    loads[1].wait()
    last = [basis[t, NB - NVEC :, :] for t in range(TD)]
    first = [dot(last[t], smooth[t]).astype(BF16) for t in range(TD)]

    def fill(r, tiles):
        for t in range(TD):
            vals[r, t] = tiles[t]
            ext[r][t] = tiles[t]

        for k in range(NF):
            pz = lax.rem(z + away(k), nz)
            for px in range(NX):
                far_tiles[r, k, px] = vals[r, member_send[pz * NX + px]]
        for j, dz in enumerate(near):
            pz = lax.rem(z + dz, nz)
            for px in range(NX):
                out_tiles[r, px, j] = vals[r, member_send[pz * NX + px]]
            turn[r][x, j] = vals[r, member_send[pz * NX + x]]
        for s in range(GG):
            out_rim[r, s] = vals[r, group_send[s]]

    def send_tiles(r):
        each_far(
            lambda k, pz, px: pltpu.make_async_remote_copy(
                src_ref=far_tiles.at[r, k, px],
                dst_ref=ext[r].at[TD + m],
                send_sem=ex_send.at[r],
                recv_sem=ex_recv.at[r],
                device_id=at_member(pz, px),
                device_id_type=MESH,
            ).start()
        )
        for d in x_order:
            pltpu.make_async_remote_copy(
                src_ref=out_tiles.at[r, xs[d]],
                dst_ref=turn[r].at[x],
                send_sem=turn_send.at[r],
                recv_sem=turn_recv.at[r],
                device_id=at_member(z, xs[d]),
                device_id_type=MESH,
            ).start()
        for step, base in ((1, TD + members), (groups - 1, TD + members + GG)):
            pltpu.make_async_remote_copy(
                src_ref=out_rim.at[r],
                dst_ref=ext[r].at[pl.ds(base, GG)],
                send_sem=ex_send.at[r],
                recv_sem=ex_recv.at[r],
                device_id={"group": lax.rem(g + step, groups), "member": m},
                device_id_type=MESH,
            ).start()

    moved = members - NX + 2 * GG

    def take_tiles(r):
        view = turn[r].at[pl.ds(0, NX - 1)]
        pltpu.make_async_copy(view, view, turn_recv.at[r]).wait()

        for j, dz in enumerate(near[:-1]):
            pltpu.make_async_remote_copy(
                src_ref=turn[r].at[:, j],
                dst_ref=ext[r].at[pl.ds(TD + z * NX, NX)],
                send_sem=ex_send.at[r],
                recv_sem=ex_recv.at[r],
                device_id=at_member(lax.rem(z + dz, nz), x),
                device_id_type=MESH,
            ).start()
        for px in range(NX):
            ext[r][TD + z * NX + px] = turn[r][px, len(near) - 1]
        view = ext[r].at[pl.ds(0, moved)]
        pltpu.make_async_copy(view, view, ex_recv.at[r]).wait()

        @pl.when(g == 0)
        def _():
            ext[r][TD + members : TD + members + GG] = jnp.zeros((GG, NVEC, TILE), BF16)

        @pl.when(g == groups - 1)
        def _():
            ext[r][TD + members + GG : TD + members + 2 * GG] = jnp.zeros((GG, NVEC, TILE), BF16)

    def operate(r, tiles):
        result = []
        for t in range(TD):
            picked = jnp.concatenate([ext[r][off_cols[t, k]] for k in range(K)], axis=1)
            result.append(dot(tiles[t], diag[t]) + dot(picked, off[t]))
        return result

    def push(i, src, dst, device):
        pltpu.make_async_remote_copy(
            src_ref=src,
            dst_ref=dst,
            send_sem=st_send.at[i],
            recv_sem=st_recv.at[i],
            device_id=device,
            device_id_type=MESH,
        ).start()

    def take(i, buf, count):
        view = buf.at[pl.ds(0, count)]
        pltpu.make_async_copy(view, view, st_recv.at[i]).wait()

    def send_x(i, own, buf):
        for d in x_order:
            push(i, own, buf.at[x], at_member(z, xs[d]))

    def send_z(i, own, buf):
        def step(k, carry):
            push(i, own, buf.at[z], at_member(z_of(k), x))
            return carry

        lax.fori_loop(0, nz - 1, step, 0)

    def send_g(i, own, buf):
        each_group(lambda pg: push(i, own, buf.at[g], {"group": pg, "member": m}))

    def total(buf, count):
        result = buf[0]
        for j in range(1, count):
            result = result + buf[j]
        return result

    loads[6].wait()
    loads[7].wait()
    fill(0, first)

    lanes = lax.broadcasted_iota(jnp.int32, (NVEC, TILE), 1)
    packed = jnp.zeros((NVEC, TILE), F32)
    for a in range(NB // NVEC):
        rows = jnp.zeros((NVEC, TILE), F32)
        for t in range(TD):
            whole = basis[t]
            four = jnp.concatenate([whole] * (TILE // NB), axis=0)
            rows = rows + dot_nt(basis[t, NVEC * a : NVEC * (a + 1), :], four)
        packed = jnp.where(lax.div(lanes, NB) == a, rows, packed)
    packed = packed * scale_rows
    b_own[...] = packed
    bz[z] = packed
    for i in (2, 3, 4, 5, 8, 9):
        loads[i].wait()

    pl.semaphore_wait(barrier, NF * NX + len(near) + NX + groups - 3)
    send_tiles(0)
    take_tiles(0)

    pieces = []
    applied = operate(0, first)
    for t in range(TD):
        residual = (last[t].astype(F32) - applied[t]).astype(BF16)
        pieces.append(dot_nt(residual, prolong[t]))
    part = []
    for a in range(CTG):
        part.append(
            sum(jnp.where(agg_map[t] == a, pieces[t], jnp.zeros_like(pieces[t])) for t in range(TD))
        )
    part = jnp.concatenate(part, axis=0)
    c_own[...] = part
    cx[x] = part
    send_x(0, c_own, cx)
    take(0, cx, NX - 1)
    part = total(cx, NX)
    s_own[...] = part
    cz[z] = part
    send_z(1, s_own, cz)

    take(1, cz, nz - 1)
    part = total(cz, nz).astype(BF16)
    for a in range(CTG):
        g_own[a] = part[NVEC * a : NVEC * (a + 1), :]
        cg[g, a] = part[NVEC * a : NVEC * (a + 1), :]
    send_g(2, g_own, cg)
    send_z(3, b_own, bz)

    take(2, cg, groups - 1)
    coarse = jnp.concatenate([cg[c // CTG, c % CTG] for c in range(groups * CTG)], axis=1)
    correction = dot(coarse, inv[...]).astype(BF16)
    for a in range(CTG):
        corr[a] = correction[:, TILE * a : TILE * (a + 1)]
    second = []
    for t in range(TD):
        second.append((first[t].astype(F32) + dot(corr[agg_map[t]], prolong[t])).astype(BF16))
    fill(1, second)
    send_tiles(1)
    take(3, bz, nz - 1)
    part = total(bz, nz)
    b2_own[...] = part
    bx[x] = part
    send_x(4, b2_own, bx)
    take_tiles(1)

    applied = operate(1, second)
    precond = []
    for t in range(TD):
        residual = (last[t].astype(F32) - applied[t]).astype(BF16)
        precond.append((second[t].astype(F32) + dot(residual, smooth[t])).astype(BF16))
    fill(2, precond)
    send_tiles(2)
    for t in range(TD):
        prec_ref[t] = precond[t]

    take(4, bx, NX - 1)
    part = total(bx, NX)
    b3_own[...] = part
    bg[g] = part
    send_g(5, b3_own, bg)
    take_tiles(2)

    applied = [value.astype(BF16) for value in operate(2, precond)]
    part = jnp.zeros((NVEC, TILE), F32)
    for t in range(TD):
        right = jnp.concatenate(
            [basis[t], applied[t], jnp.zeros((TILE - NB - NVEC, TILE), BF16)], axis=0
        )
        part = part + dot_nt(applied[t], right)
    part = part * scale_rows
    f_own[...] = part
    fg[g] = part
    send_g(6, f_own, fg)
    take(6, fg, groups - 1)
    part = total(fg, groups)
    part = part[:3] + pltpu.roll(part[3:6], 40, 1) + pltpu.roll(part[5:], 80, 1)
    f2_own[...] = part
    fx[x] = part
    each_far(lambda k, pz, px: push(9, f2_own, ff.at[m], at_member(pz, px)))
    send_x(7, f2_own, fx)
    take(5, bg, groups - 1)
    packed = total(bg, groups)
    basis_total = jnp.concatenate(
        [
            packed if a == 0 else pltpu.roll(packed, TILE - NB * a, 1)
            for a in range(NB // NVEC)
        ],
        axis=0,
    )
    wide_lanes = lax.broadcasted_iota(jnp.int32, (NB, TILE), 1)
    wide_rows = lax.broadcasted_iota(jnp.int32, (NB, TILE), 0)
    basis_total = jnp.where(wide_lanes < NB, basis_total, 0.0)
    mirror = jnp.where(wide_rows == wide_lanes, 2.0, 0.0) - basis_total
    take(7, fx, NX - 1)
    part = total(fx, NX)
    f3_own[...] = part
    for dz in near[:-1]:
        push(8, f3_own, fz.at[z], at_member(lax.rem(z + dz, nz), x))
    fz[z] = part
    take(9, ff, NF * NX)
    for k in range(NF):
        pz = lax.rem(z + away(k), nz)
        fz_sum = ff[pz * NX]
        for px in range(1, NX):
            fz_sum = fz_sum + ff[pz * NX + px]
        fold[pz] = fz_sum
    take(8, fz, len(near) - 1)
    fold[z] = part
    for dz in near[:-1]:
        pz = lax.rem(z + dz, nz)
        fold[pz] = fz[pz]
    part = total(fold, nz)
    whole = jnp.concatenate([part, pltpu.roll(part, 88, 1), pltpu.roll(part, 48, 1)[1:]], axis=0)
    part = whole

    coef = jnp.where(lanes < NB, part, 0.0)
    square = pltpu.roll(part, TILE - NB, 1)
    coef_ref[...] = part[:, :NB]
    narrow = coef[:, :NB]
    gram = square[:, :NVEC] - exact_nt(exact(narrow, mirror), coef)
    gram_ref[...] = gram
    rest = [applied[t].astype(F32) - exact(narrow, basis[t].astype(F32)) for t in range(TD)]
    ids = lax.broadcasted_iota(jnp.int32, (NVEC, 1), 0)
    left = gram
    for j in range(NVEC - 1):
        pivot_row = left[j : j + 1, :]
        factor = left[:, j : j + 1] / left[j : j + 1, j : j + 1]
        factor = jnp.where(ids > j, factor, 0.0)
        left = left - factor * pivot_row
        rest = [r - factor * r[j : j + 1, :] for r in rest]
    row_ids = lax.broadcasted_iota(jnp.int32, (NVEC, NVEC), 0)
    col_ids = lax.broadcasted_iota(jnp.int32, (NVEC, NVEC), 1)
    pivots = jnp.sum(jnp.where(row_ids == col_ids, left, 0.0), axis=1, keepdims=True)
    gain = 1.0 / jnp.sqrt(pivots)
    for t in range(TD):
        new_ref[t] = rest[t] * gain

    for r in range(3):
        view = ext[r].at[pl.ds(0, moved)]
        pltpu.make_async_copy(view, view, ex_send.at[r]).wait()
        view = turn[r].at[pl.ds(0, NX - 1)]
        pltpu.make_async_copy(view, view, turn_send.at[r]).wait()
    for i, (buf, count) in enumerate(
        (
            (cx, NX), (cz, nz), (cg, groups), (bz, nz), (bx, NX), (bg, groups),
            (fg, groups), (fx, NX), (fz, len(near)), (ff, NF * NX + 1),
        )
    ):
        view = buf.at[pl.ds(0, count - 1)]
        pltpu.make_async_copy(view, view, st_send.at[i]).wait()


def finish(*refs):
    sem = refs[8]
    copies = [pltpu.make_async_copy(refs[i], refs[4 + i], sem.at[i]) for i in range(4)]
    for copy in copies:
        copy.start()
    for copy in copies:
        copy.wait()


def local(groups, members, off_tiles, off_cols, member_send, group_send, diag_tiles, smoother,
          agg_map, prolong, coarse_inv, krylov_basis):
    nz = members // NX
    rows_all = TD * TILE * members * groups
    hbm = pl.BlockSpec(memory_space=pltpu.HBM)
    vmem = pl.BlockSpec(memory_space=pltpu.VMEM)
    slots = TD + members + 2 * GG
    wide = (NVEC, TILE)
    call = pl.pallas_call(
        functools.partial(cycle, groups, members, rows_all),
        out_shape=(
            jax.ShapeDtypeStruct((TD, NVEC, TILE), BF16),
            jax.ShapeDtypeStruct((NVEC, NB), F32),
            jax.ShapeDtypeStruct((NVEC, NVEC), F32),
            jax.ShapeDtypeStruct((TD, NVEC, TILE), F32),
        ),
        in_specs=[hbm] * 10,
        out_specs=(vmem,) * 4,
        scratch_shapes=[
            pltpu.SMEM((TD, K), jnp.int32),
            pltpu.SMEM((members,), jnp.int32),
            pltpu.SMEM((GG,), jnp.int32),
            pltpu.SMEM((TD,), jnp.int32),
            pltpu.VMEM((TD, K * TILE, TILE), BF16),
            pltpu.VMEM((TD, TILE, TILE), BF16),
            pltpu.VMEM((TD, TILE, TILE), BF16),
            pltpu.VMEM((TD, TILE, TILE), BF16),
            pltpu.VMEM((groups * CTG * TILE, CTG * TILE), BF16),
            pltpu.VMEM((TD, NB, TILE), BF16),
            pltpu.VMEM((3, TD, NVEC, TILE), BF16),
            pltpu.VMEM((3, NF, NX, NVEC, TILE), BF16),
            pltpu.VMEM((3, NX, nz - NF, NVEC, TILE), BF16),
            pltpu.VMEM((3, GG, NVEC, TILE), BF16),
            pltpu.VMEM((NX, nz - NF, NVEC, TILE), BF16),
            pltpu.VMEM((NX, nz - NF, NVEC, TILE), BF16),
            pltpu.VMEM((NX, nz - NF, NVEC, TILE), BF16),
            pltpu.VMEM((slots, NVEC, TILE), BF16),
            pltpu.VMEM((slots, NVEC, TILE), BF16),
            pltpu.VMEM((slots, NVEC, TILE), BF16),
            pltpu.VMEM((NX, CTG * NVEC, TILE), F32),
            pltpu.VMEM((nz, CTG * NVEC, TILE), F32),
            pltpu.VMEM((groups, CTG, NVEC, TILE), BF16),
            pltpu.VMEM((CTG, NVEC, TILE), BF16),
            pltpu.VMEM((nz, *wide), F32),
            pltpu.VMEM((NX, *wide), F32),
            pltpu.VMEM((groups, *wide), F32),
            pltpu.VMEM((groups, *wide), F32),
            pltpu.VMEM((NX, 3, TILE), F32),
            pltpu.VMEM((members, 3, TILE), F32),
            pltpu.VMEM((nz, 3, TILE), F32),
            pltpu.VMEM((nz, 3, TILE), F32),
            pltpu.VMEM((CTG * NVEC, TILE), F32),
            pltpu.VMEM((CTG * NVEC, TILE), F32),
            pltpu.VMEM((CTG, NVEC, TILE), BF16),
            pltpu.VMEM(wide, F32),
            pltpu.VMEM(wide, F32),
            pltpu.VMEM(wide, F32),
            pltpu.VMEM(wide, F32),
            pltpu.VMEM((3, TILE), F32),
            pltpu.VMEM((3, TILE), F32),
            pltpu.SemaphoreType.DMA((10,)),
            pltpu.SemaphoreType.DMA((3,)),
            pltpu.SemaphoreType.DMA((3,)),
            pltpu.SemaphoreType.DMA((3,)),
            pltpu.SemaphoreType.DMA((3,)),
            pltpu.SemaphoreType.DMA((10,)),
            pltpu.SemaphoreType.DMA((10,)),
        ],
        compiler_params=pltpu.CompilerParams(
            collective_id=0, has_side_effects=True, vmem_limit_bytes=16 << 20
        ),
        name="cycle",
    )
    arrays = (
        off_cols,
        member_send.reshape(members),
        group_send.reshape(GG),
        agg_map,
        off_tiles.reshape(TD, K * TILE, TILE),
        diag_tiles,
        smoother,
        prolong,
        coarse_inv,
        krylov_basis,
    )
    results = call(*(pltpu.with_memory_space_constraint(v, pltpu.HBM) for v in arrays))
    hand_out = pl.pallas_call(
        finish,
        out_shape=tuple(jax.ShapeDtypeStruct(r.shape, r.dtype) for r in results),
        in_specs=[vmem] * 4,
        out_specs=(hbm,) * 4,
        scratch_shapes=[pltpu.SemaphoreType.DMA((4,))],
        compiler_params=pltpu.CompilerParams(vmem_limit_bytes=1 << 20),
        name="finish",
    )
    precond, coef, gram, new_block = hand_out(*results)
    return precond, coef.T, gram, new_block


def solution(mesh):
    groups, members = mesh.shape["group"], mesh.shape["member"]
    both = ("group", "member")
    in_specs = (
        P(both, None, None, None),
        P(both, None),
        P(both, None, None),
        P(both, None),
        P(both, None, None),
        P(both, None, None),
        P(both),
        P(both, None, None),
        P(None, "group"),
        P(both, None, None),
    )
    out_specs = (P(both, None, None), P(), P(), P(both, None, None))
    return jax.shard_map(
        functools.partial(local, groups, members),
        mesh=mesh,
        in_specs=in_specs,
        out_specs=out_specs,
        check_vma=False,
    )
```
